32 devices in a mesh: ex: 8 (over y, x, core), tp: 4 (over z).
Axes of the slice: x: 2, y: 2, z: 4, core: 2. Of those that a mesh axis runs over, the one named last changes fastest.
Arguments:
- samples: bfloat16 [192, 2048], P(('ex', 'tp')), may hold values from -6 to 6
- gate_weight: bfloat16 [2048, 44], replicated, may hold values from -15 to 15
- up_weight: bfloat16 [16, 2048, 4096], P('ex', None, 'tp'), may hold values from -0.125 to 0.125
- down_weight: bfloat16 [16, 4096, 2048], P('ex', 'tp'), may hold values from -0.09375 to 0.09375
Outputs:
- task_outputs: bfloat16 [192, 5, 2048], P(('ex', 'tp'))
The draws below stay inside these ranges and needn't reach their ends.
All inputs are finite; a program needn't handle non-finite values.
Results may differ from the reference program's by a relative error of at most 0.0055.
Values may be sent and summed in bfloat16 or wider, within the bound.
A program may use at most 128 MiB of HBM per device.

```python
import jax
import jax.numpy as jnp
import numpy as np
from jax import lax

D = 2048
FF = 4096
TASKS = 4
TASK_EXP = 3
SHARED = 4
EXPERTS = 16
GATES = 44
ROWS = 192


def draw_gate_weight(key, part):
    first_key = jax.random.fold_in(key, 11)
    base = jax.random.normal(first_key, (D, GATES), jnp.float32)
    values = base * (2.0 / jnp.sqrt(jnp.float32(D)))
    return jnp.clip(values, -15.0, 15.0).astype(jnp.bfloat16)


def levels(own_key, extent, shards, low, high):
    gain = 1.0
    for axis_at, shards_of in shards:
        heights = jax.random.uniform(jax.random.fold_in(jax.random.fold_in(own_key, 6), axis_at), (shards_of,), jnp.float32, low / len(shards), high / len(shards))
        gain = gain * jnp.repeat(jnp.exp(heights), extent[axis_at] // shards_of).reshape((-1,) + (1,) * (len(extent) - 1 - axis_at))
    return gain


def scatter_about(rng, extent, scale, limit, split=(), held_as=jnp.bfloat16):
    values = scale * jax.random.normal(rng, extent, jnp.float32)
    if split:
        values = values * levels(rng, extent, split, -0.22, 0.18)
    return jnp.clip(values, -limit, limit).astype(held_as)


def setup_inputs(seed: int = 0) -> dict:
    seeds = jax.random.split(jax.random.key(seed), 5)
    samples = scatter_about(seeds[0], (ROWS, D), 1.0, 6.0, ((0, 32),))
    gate_weight = draw_gate_weight(jax.random.fold_in(seeds[4], 71), 0)
    up_weight = scatter_about(seeds[2], (EXPERTS, D, FF), D ** -0.5, 0.125, ((0, 8), (2, 4)))
    down_weight = scatter_about(seeds[3], (EXPERTS, FF, D), FF ** -0.5, 0.09375, ((0, 8), (1, 4)))
    return dict(samples=samples, gate_weight=gate_weight, up_weight=up_weight, down_weight=down_weight)


def routing_table():
    per_task = TASK_EXP + SHARED
    table = np.zeros((GATES, (TASKS + 1) * EXPERTS), np.float32)
    for task_idx in range(TASKS):
        for column in range(per_task):
            if column < TASK_EXP:
                expert_idx = task_idx * TASK_EXP + column
            else:
                expert_idx = TASKS * TASK_EXP + column - TASK_EXP
            table[task_idx * per_task + column, task_idx * EXPERTS + expert_idx] = 1.0
    for expert_idx in range(EXPERTS):
        table[TASKS * per_task + expert_idx, TASKS * EXPERTS + expert_idx] = 1.0
    return jnp.asarray(table, dtype=jnp.float32)


def gate_mix(rows, gate_weight):
    logits = jnp.dot(rows, gate_weight, preferred_element_type=jnp.float32)
    per_task = TASK_EXP + SHARED
    pieces = []
    for task_idx in range(TASKS):
        pieces.append(jax.nn.softmax(logits[:, task_idx * per_task:(task_idx + 1) * per_task], axis=-1))
    pieces.append(jax.nn.softmax(logits[:, TASKS * per_task:], axis=-1))
    probs = jnp.concatenate(pieces, axis=1)
    mixed = jnp.dot(probs, routing_table(), precision=lax.Precision.HIGHEST)
    return mixed.reshape(rows.shape[0], TASKS + 1, EXPERTS)


def reference(samples, gate_weight, up_weight, down_weight):
    mixing = gate_mix(samples, gate_weight)
    weights_by_expert = jnp.transpose(mixing, (2, 0, 1))

    def accumulate(total, item):
        first, second, weighs = item
        hidden = jnp.maximum(jnp.dot(samples, first, preferred_element_type=jnp.float32), 0.0).astype(jnp.bfloat16)
        expert_out = jnp.dot(hidden, second, preferred_element_type=jnp.float32)
        return total + weighs[:, :, None] * expert_out[:, None, :], None

    start_total = jnp.zeros((samples.shape[0], TASKS + 1, samples.shape[1]), jnp.float32)
    total, unused = lax.scan(accumulate, start_total, (up_weight, down_weight, weights_by_expert))
    return total.astype(jnp.bfloat16)
```

```python
import functools

import jax
import jax.numpy as jnp
import numpy as np
from jax import lax
from jax.experimental import pallas as pl
from jax.experimental.pallas import tpu as pltpu
from jax.sharding import PartitionSpec as P

TASKS = 4
TASK_EXP = 3
SHARED = 4
EXPERTS = 16
GATES = 44
OUTS = TASKS + 1
SLAB = 8
LANES = 128
MESH = pl.DeviceIdType.MESH


def column_facts():
    per_task = TASK_EXP + SHARED
    gate_of = np.full(LANES, -1)
    expert_of = np.full(LANES, -1)
    for column in range(TASKS * per_task):
        task_idx, j = divmod(column, per_task)
        gate_of[column] = task_idx
        expert_of[column] = (
            task_idx * TASK_EXP + j if j < TASK_EXP else TASKS * TASK_EXP + j - TASK_EXP
        )
    for expert_idx in range(EXPERTS):
        gate_of[TASKS * per_task + expert_idx] = TASKS
        expert_of[TASKS * per_task + expert_idx] = expert_idx
    return gate_of, expert_of


def constants(ex, tp, rows, experts, group):
    block = tp * rows
    out_rows = pad16(rows * OUTS)
    pack = np.zeros((group * rows, group * SLAB), np.float32)
    for slab in range(group):
        for r in range(rows):
            pack[slab * rows + r, slab * SLAB + r] = 1.0
    gate_of, expert_of = column_facts()
    total = tp * out_rows
    repeat = np.zeros((total, tp * SLAB), np.float32)
    mask = np.zeros((total, LANES), np.float32)
    column_expert = np.repeat(np.arange(ex * experts), block)
    column_row = np.tile(np.arange(block), ex * experts)
    spread = (expert_of[:, None] == column_expert[None, :]).astype(np.float32)
    match = np.zeros((total, ex * experts * block), np.float32)
    for t in range(tp):
        for q in range(out_rows):
            i = t * out_rows + q
            r, k = divmod(q, OUTS)
            if r < rows:
                repeat[i, t * SLAB + r] = 1.0
                mask[i] = gate_of == k
                match[i] = column_row == t * rows + r
            else:
                mask[i] = gate_of == TASKS
    return (
        jnp.asarray(pack, jnp.bfloat16),
        jnp.asarray(repeat, jnp.float32),
        jnp.asarray(mask, jnp.float32),
        jnp.asarray(spread, jnp.bfloat16),
        jnp.asarray(match, jnp.bfloat16),
    )


def pad16(n):
    return -(-n // 16) * 16


def kernel(
    ex, tp, chunks, group,
    x_ref, gate_ref, pack_ref, repeat_ref, mask_ref, spread_ref, match_ref, up_hbm, down_hbm,
    out_ref,
    slabs, packed, up, down, hidden, mix, send1, recv1, send2, recv2,
    up_sem, down_sem, tp_send, ex_send, sib_send, slab_recv, s1_send, s1_recv, s2_send, s2_recv,
):
    e, t = lax.axis_index("ex"), lax.axis_index("tp")
    rows, width = x_ref.shape
    experts, _, ff = up_hbm.shape
    block = tp * rows
    part = width // chunks
    half = ex // 2
    out_rows = recv2.shape[2]
    total = tp * out_rows

    up_copies = [
        pltpu.make_async_copy(up_hbm.at[l], up.at[l], up_sem.at[l]) for l in range(experts)
    ]
    down_copies = [
        pltpu.make_async_copy(down_hbm.at[l], down.at[l], down_sem.at[l]) for l in range(experts)
    ]
    for copy in up_copies + down_copies:
        copy.start()

    barrier = pltpu.get_barrier_semaphore()
    for d in range(1, tp):
        pl.semaphore_signal(
            barrier, inc=1, device_id=(e, lax.rem(t + d, tp)), device_id_type=MESH
        )
    for d in range(1, ex):
        pl.semaphore_signal(
            barrier, inc=1, device_id=(lax.rem(e + d, ex), t), device_id_type=MESH
        )
    mine = e * tp + t
    slabs[mine, :rows, :] = x_ref[...]
    slabs[mine, rows:, :] = jnp.zeros((SLAB - rows, width), jnp.bfloat16)
    pl.semaphore_wait(barrier, tp - 1 + ex - 1)

    core = lax.rem(e, 2)
    sibling = e + 1 - 2 * core

    def slab_copy(slab, send_sem, device):
        return pltpu.make_async_remote_copy(
            src_ref=slabs.at[slab],
            dst_ref=slabs.at[slab],
            send_sem=send_sem,
            recv_sem=slab_recv.at[slab],
            device_id=device,
            device_id_type=MESH,
        )

    started = []
    for d in range(1, tp):
        copy = slab_copy(mine, tp_send.at[d], (e, lax.rem(t + d, tp)))
        copy.start()
        started.append(copy)
    for step in range(tp):
        slab = e * tp + lax.rem(t + step, tp)
        if step:
            slab_copy(slab, tp_send.at[step], (e, t)).wait_recv()
        for d in range(1, half):
            copy = slab_copy(slab, ex_send.at[step, d], (lax.rem(e + 2 * d, ex), t))
            copy.start()
            started.append(copy)
        copy = slab_copy(slab, sib_send.at[0, step], (sibling, t))
        copy.start()
        started.append(copy)
    for step in range(tp):
        for d in range(1, half):
            slab = lax.rem(e + 2 * d, ex) * tp + lax.rem(t + step, tp)
            slab_copy(slab, ex_send.at[step, d], (e, t)).wait_recv()
            copy = slab_copy(slab, sib_send.at[d, step], (sibling, t))
            copy.start()
            started.append(copy)

    own = slabs[pl.ds(e * tp, tp)].astype(jnp.float32).reshape(tp * SLAB, width)
    logits = jnp.dot(
        own.astype(jnp.bfloat16), gate_ref[...], preferred_element_type=jnp.float32
    )
    logits = jnp.concatenate(
        [logits, jnp.zeros((tp * SLAB, LANES - GATES), jnp.float32)], axis=1
    )
    logits = jnp.dot(
        repeat_ref[...], logits, precision=lax.Precision.HIGHEST,
        preferred_element_type=jnp.float32,
    )
    chosen = mask_ref[...] > 0.0
    logits = jnp.where(chosen, logits, -jnp.inf)
    powers = jnp.exp(logits - jnp.max(logits, axis=1, keepdims=True))
    probs = powers / jnp.sum(powers, axis=1, keepdims=True)
    high = probs.astype(jnp.bfloat16)
    low = (probs - high.astype(jnp.float32)).astype(jnp.bfloat16)
    match = match_ref[...].astype(jnp.float32)
    for at, piece in ((0, high), (total, low)):
        placed = jnp.dot(piece, spread_ref[...], preferred_element_type=jnp.float32)
        mix[at : at + total, :] = (placed * match).astype(jnp.bfloat16)

    for step in range(tp):
        for d in range(half):
            slab = lax.rem(sibling + 2 * d, ex) * tp + lax.rem(t + step, tp)
            slab_copy(slab, sib_send.at[d, step], (e, t)).wait_recv()

    slabs_all = ex * tp
    for g in range(slabs_all // group):
        raw = slabs[g * group : (g + 1) * group].astype(jnp.float32)
        raw = raw.reshape(group * SLAB, width).astype(jnp.bfloat16)
        packed[g * group * rows : (g + 1) * group * rows, :] = jnp.dot(
            pack_ref[...], raw, preferred_element_type=jnp.float32
        ).astype(jnp.bfloat16)

    tile = min(256, ff)
    for l in range(experts):
        up_copies[l].wait()

        def up_step(i, carry, l=l):
            cols = pl.ds(pl.multiple_of(i * tile, tile), tile)
            value = jnp.dot(packed[...], up[l, :, cols], preferred_element_type=jnp.float32)
            hidden[l, :, cols] = jnp.maximum(value, 0.0).astype(jnp.bfloat16)
            return carry

        lax.fori_loop(0, ff // tile, up_step, 0)

    for copy in down_copies:
        copy.wait()

    def first_copy(c, dest, d, source_slot):
        return pltpu.make_async_remote_copy(
            src_ref=send1.at[c, dest],
            dst_ref=recv1.at[c, source_slot],
            send_sem=s1_send.at[c, d],
            recv_sem=s1_recv.at[c, source_slot],
            device_id=(dest, t),
            device_id_type=MESH,
        )

    def down_step(c, carry):
        cols = pl.ds(pl.multiple_of(c * part, part), part)
        values = [
            jnp.dot(hidden[l], down[l, :, cols], preferred_element_type=jnp.float32)
            for l in range(experts)
        ]
        for dest in range(ex):
            pieces = [v[dest * block : (dest + 1) * block] for v in values]
            joined = jnp.concatenate(pieces, axis=0) if experts > 1 else pieces[0]
            send1[c, dest] = joined.astype(jnp.bfloat16)
        for d in range(1, ex):
            first_copy(c, lax.rem(e + d, ex), d, e).start()
        recv1[c, e] = send1[c, e]
        return carry

    lax.fori_loop(0, chunks, down_step, 0)

    def second_copy(c, dest, d, source_slot):
        return pltpu.make_async_remote_copy(
            src_ref=send2.at[c, dest],
            dst_ref=recv2.at[c, source_slot],
            send_sem=s2_send.at[c, d],
            recv_sem=s2_recv.at[c, source_slot],
            device_id=(e, dest),
            device_id_type=MESH,
        )

    def mix_step(c, carry):
        for d in range(1, ex):
            first_copy(c, e, d, lax.rem(e + d, ex)).wait_recv()
        got = recv1[c].reshape(ex * experts * block, part)
        both = jnp.dot(mix[...], got, preferred_element_type=jnp.float32)
        mixed = (both[:total] + both[total:]).astype(jnp.bfloat16)
        for dest in range(tp):
            send2[c, dest] = mixed[dest * out_rows : (dest + 1) * out_rows]
        for d in range(1, tp):
            second_copy(c, lax.rem(t + d, tp), d, t).start()
        return carry

    lax.fori_loop(0, chunks, mix_step, 0)

    for c in range(chunks):
        sum_ = send2[c, t].astype(jnp.float32)
        for d in range(1, tp):
            source = lax.rem(t + d, tp)
            second_copy(c, t, d, source).wait_recv()
            sum_ = sum_ + recv2[c, source].astype(jnp.float32)
        out_ref[:, c * part : (c + 1) * part] = sum_.astype(jnp.bfloat16)

    for copy in started:
        copy.wait_send()

    def drain(c, carry):
        for d in range(1, ex):
            first_copy(c, lax.rem(e + d, ex), d, e).wait_send()
        for d in range(1, tp):
            second_copy(c, lax.rem(t + d, tp), d, t).wait_send()
        return carry

    lax.fori_loop(0, chunks, drain, 0)


def on_device(ex, tp, samples, gate_weight, up_weight, down_weight):
    experts, width, ff = up_weight.shape
    rows = samples.shape[0]
    block = tp * rows
    chunks = 4
    part = width // chunks
    group = min(32, ex * tp)
    out_rows = pad16(rows * OUTS)
    tables = constants(ex, tp, rows, experts, group)
    bf16 = jnp.bfloat16
    dma = pltpu.SemaphoreType.DMA
    vmem = pl.BlockSpec(memory_space=pltpu.VMEM)
    hbm = pl.BlockSpec(memory_space=pl.ANY)
    result = pl.pallas_call(
        functools.partial(kernel, ex, tp, chunks, group),
        out_shape=jax.ShapeDtypeStruct((out_rows, width), bf16),
        in_specs=[vmem] * 7 + [hbm] * 2,
        out_specs=vmem,
        scratch_shapes=[
            pltpu.VMEM((ex * tp, SLAB, width), bf16),
            pltpu.VMEM((ex * tp * rows, width), bf16),
            pltpu.VMEM((experts, width, ff), bf16),
            pltpu.VMEM((experts, ff, width), bf16),
            pltpu.VMEM((experts, ex * tp * rows, ff), bf16),
            pltpu.VMEM((2 * tp * out_rows, ex * experts * block), bf16),
            pltpu.VMEM((chunks, ex, experts * block, part), bf16),
            pltpu.VMEM((chunks, ex, experts * block, part), bf16),
            pltpu.VMEM((chunks, tp, out_rows, part), bf16),
            pltpu.VMEM((chunks, tp, out_rows, part), bf16),
            dma((experts,)),
            dma((experts,)),
            dma((tp,)),
            dma((tp, ex // 2)),
            dma((ex // 2, tp)),
            dma((ex * tp,)),
            dma((chunks, ex)),
            dma((chunks, ex)),
            dma((chunks, tp)),
            dma((chunks, tp)),
        ],
        compiler_params=pltpu.CompilerParams(
            collective_id=0, has_side_effects=True, vmem_limit_bytes=63_000_000
        ),
    )(samples, gate_weight, *tables, up_weight, down_weight)
    return result[: rows * OUTS].reshape(rows, OUTS, width)


def solution(mesh):
    placed = (P(("ex", "tp"), None), P(), P("ex", None, "tp"), P("ex", "tp", None))
    return jax.shard_map(
        functools.partial(on_device, mesh.shape["ex"], mesh.shape["tp"]),
        mesh=mesh,
        in_specs=placed,
        out_specs=P(("ex", "tp"), None, None),
        check_vma=False,
    )
```
